32 devices in a mesh: member: 2 (over x), dp: 8 (over z, y), mp: 2 (over core).
Axes of the slice: x: 2, y: 2, z: 4, core: 2. Of those that a mesh axis runs over, the one named last changes fastest.
Arguments:
- activations: bfloat16 [2048, 2048], P(('member', 'dp')), parts along dimension 0, may hold values from -6 to 6
- out_grads: bfloat16 [2048, 10240], P(('member', 'dp'), 'mp'), parts along dimension 0, may hold values from -0.19921875 to 0.19921875
- slot_table: int32 [4, 16], P(('member', 'mp')), parts along dimension 0, may hold values from 0 to 15, each once within a row
- exponent_index: int32 [4, 16], P(('member', 'mp')), parts along dimension 0, may hold values from 0 to 1
- damping_index: int32 [4, 16], P(('member', 'mp')), parts along dimension 0, may hold values from 0 to 3
Outputs:
- update: bfloat16 [4096, 10240], P('member', 'mp'), parts along dimension 0
- preconditioners: bfloat16 [4, 16, 2, 1024, 1024], P(('member', 'mp'), 'dp'), parts along dimension 0
The draws below stay inside these ranges and needn't reach their ends.
There are 2 independent parts, one for each index of `member`. The reference program is written for one: setup_inputs(seed, part) draws one part's arguments, and reference() takes and returns one part's arrays. A program takes and returns all parts, laid end to end along the dimension named above; each array names one. Nothing has to cross between parts.
Inputs may be any that keep to these rules, and one draw needn't show every extreme that they name: `slot_table`: each row is a permutation of 0 to 15; slot s belongs to dp index s.
All inputs are finite; a program needn't handle non-finite values.
Results may differ from the reference program's by a relative error of at most 0.006.
The reference program's roundings to bfloat16 on the way (of `gradient`, `half_step` and `assembled`) count: a program that leaves them out, or rounds other values in their place, can miss the bound.
Values may be sent and summed in bfloat16 or wider, within the bound.
A program may use at most 192 MiB of HBM per device.

```python
import jax
import jax.numpy as jnp
from jax import lax

D_WIN = 2048
FF_WIN = 10240
BLK = 1024
SLOTS = 16
ITERS = 2
TOKENS = 1024
N_MP = 2


def plant(entries, stream_key, least, top_value):
    index_at = [jax.random.randint(jax.random.fold_in(stream_key, axis), (), 0, length) for axis, length in enumerate(entries.shape)]
    widest = entries.shape.index(max(entries.shape))
    neighbour = index_at[:widest] + [(index_at[widest] + 1) % entries.shape[widest]] + index_at[widest + 1:]
    return entries.at[tuple(index_at)].set(least).at[tuple(neighbour)].set(top_value)


def block_levels(own_key, dims, cuts, low, top_value):
    factor_of, own = 1.0, jax.random.fold_in(own_key, 6)
    for dim, shards_of in cuts:
        heights = jnp.exp(jax.random.uniform(jax.random.fold_in(own, dim), (shards_of,), jnp.float32, low / len(cuts), top_value / len(cuts)))
        factor_of = factor_of * jnp.repeat(heights, dims[dim] // shards_of).reshape([-1 if axis == dim else 1 for axis in range(len(dims))])
    return factor_of


def gaussian(key, extent, width, bound, split=(), kind=jnp.bfloat16):
    array = width * jax.random.normal(key, extent, jnp.float32)
    if split:
        array = array * block_levels(key, extent, split, -0.22, 0.18)
    return jnp.clip(array, -bound, bound).astype(kind)


def setup_inputs(seed: int = 0, part: int = 0) -> dict:
    keys = jax.random.split(jax.random.key(seed), 6)
    part_keys = jax.random.split(jax.random.fold_in(keys[5], part), 6)
    activations = gaussian(part_keys[0], (TOKENS, D_WIN), 1.0, 6.0, ((0, 8),))
    out_grads = gaussian(part_keys[1], (TOKENS, FF_WIN), 0.03125, 0.19921875, ((0, 8), (1, 2)))
    slot_table = jax.vmap(lambda own: jax.random.permutation(own, SLOTS))(jax.random.split(part_keys[2], N_MP)).reshape((N_MP, SLOTS)).astype(jnp.int32)
    exponent_index = plant(jax.random.randint(part_keys[3], (N_MP, SLOTS), 0, 2), jax.random.fold_in(part_keys[3], 1), 0, 1).astype(jnp.int32)
    damping_index = plant(jax.random.randint(part_keys[4], (N_MP, SLOTS), 0, 4), jax.random.fold_in(part_keys[4], 1), 0, 3).astype(jnp.int32)
    return dict(activations=activations, out_grads=out_grads, slot_table=slot_table, exponent_index=exponent_index, damping_index=damping_index)


ROOT_ORDERS = (2.0, 4.0)
DAMPINGS = (0.03, 0.1, 0.3, 1.0)

def table_value(picked, values_table):
    values = jnp.asarray(values_table, jnp.float32)
    matches = jnp.arange(len(values_table), dtype=jnp.int32) == picked
    return jnp.sum(jnp.where(matches, values, 0.0))

def half_dot(first, second):
    return jnp.dot(first.astype(jnp.bfloat16), second.astype(jnp.bfloat16), preferred_element_type=jnp.float32)

def inverse_root(statistic, root_order, quartic, damping):
    dimension = statistic.shape[0]
    identity = jnp.eye(dimension, dtype=jnp.float32)
    damped = statistic + damping * (jnp.trace(statistic) / dimension + 1.0) * identity
    current = damped * (dimension / (2.0 * jnp.trace(damped)))
    factor = ((root_order + 1.0) * identity - current) / root_order
    estimate = factor
    for sweep in range(1, ITERS):
        square = half_dot(factor, factor)
        fourth = half_dot(square, square)
        raised = jnp.where(quartic, fourth, square)
        current = half_dot(raised, current)
        factor = ((root_order + 1.0) * identity - current) / root_order
        estimate = half_dot(estimate, factor)
    return estimate.astype(jnp.bfloat16)

def precondition(act_block, grad_block, root_order, quartic, damping):
    gradient = lax.dot_general(act_block, grad_block, (((0,), (0,)), ((), ())), preferred_element_type=jnp.float32).astype(jnp.bfloat16)
    left_stat = lax.dot_general(gradient, gradient, (((1,), (1,)), ((), ())), preferred_element_type=jnp.float32)
    right_stat = lax.dot_general(gradient, gradient, (((0,), (0,)), ((), ())), preferred_element_type=jnp.float32)
    left_root = inverse_root(left_stat, root_order, quartic, damping)
    right_root = inverse_root(right_stat, root_order, quartic, damping)
    half_step = jnp.dot(left_root, gradient, preferred_element_type=jnp.float32).astype(jnp.bfloat16)
    block_update = jnp.dot(half_step, right_root, preferred_element_type=jnp.float32).astype(jnp.bfloat16)
    return (block_update, jnp.stack([left_root, right_root]))

def reference(activations, out_grads, slot_table, exponent_index, damping_index):
    row_blocks = D_WIN // BLK
    col_blocks = FF_WIN // (N_MP * BLK)
    half_blocks = row_blocks * col_blocks
    acts_grid = activations.reshape(TOKENS, row_blocks, BLK)
    grads_grid = out_grads.reshape(TOKENS, N_MP, col_blocks, BLK)
    flat_exp = exponent_index.reshape(N_MP * SLOTS)
    flat_damp = damping_index.reshape(N_MP * SLOTS)

    def one_slot(flat_slot):
        half_id = flat_slot // SLOTS
        slot_id = flat_slot % SLOTS
        exp_pick = lax.dynamic_index_in_dim(flat_exp, flat_slot, 0, keepdims=False)
        damp_pick = lax.dynamic_index_in_dim(flat_damp, flat_slot, 0, keepdims=False)
        root_order = table_value(exp_pick, ROOT_ORDERS)
        quartic = exp_pick == 1
        damping = table_value(damp_pick, DAMPINGS)
        table_row = lax.dynamic_index_in_dim(slot_table, half_id, 0, keepdims=False)[:half_blocks]
        matches = table_row == slot_id
        filled = jnp.any(matches)
        block_id = jnp.sum(jnp.where(matches, jnp.arange(half_blocks, dtype=jnp.int32), 0)).astype(jnp.int32)
        act_block = lax.dynamic_index_in_dim(acts_grid, block_id // col_blocks, 1, keepdims=False)
        grad_half = lax.dynamic_index_in_dim(grads_grid, half_id, 1, keepdims=False)
        grad_block = lax.dynamic_index_in_dim(grad_half, block_id % col_blocks, 1, keepdims=False)
        act_block = jnp.where(filled, act_block, jnp.zeros_like(act_block))
        grad_block = jnp.where(filled, grad_block, jnp.zeros_like(grad_block))
        return precondition(act_block, grad_block, root_order, quartic, damping)
    block_updates, roots = lax.map(one_slot, jnp.arange(N_MP * SLOTS, dtype=jnp.int32))
    by_slot = block_updates.reshape(N_MP, SLOTS, BLK, BLK)
    chosen = jnp.take_along_axis(by_slot, slot_table[:, :half_blocks][:, :, None, None], axis=1)
    assembled = chosen.reshape(N_MP, row_blocks, col_blocks, BLK, BLK).transpose(1, 3, 0, 2, 4).reshape(D_WIN, FF_WIN)
    wide = assembled.astype(jnp.float32)
    total_sq = jnp.sum(wide * wide)
    rescale = lax.rsqrt(total_sq / (D_WIN * FF_WIN) + 1.0)
    update = (wide * rescale).astype(jnp.bfloat16)
    return (update, roots.reshape(N_MP, SLOTS, 2, BLK, BLK))
```

```python
import functools

import jax
import jax.numpy as jnp
from jax import lax
from jax.experimental import pallas as pl
from jax.experimental.pallas import tpu as pltpu
from jax.sharding import PartitionSpec as P

BLK = 1024
PANEL = 256
DAMPINGS = (0.03, 0.1, 0.3, 1.0)
VMEM_BYTES = 60 * 1024 * 1024

NORMAL = (((1,), (0,)), ((), ()))
LEFT_T = (((0,), (0,)), ((), ()))
RIGHT_T = (((1,), (1,)), ((), ()))
MESH = pl.DeviceIdType.MESH


def dot(lhs, rhs, dims=NORMAL):
    return lax.dot_general(lhs, rhs, dims, preferred_element_type=jnp.float32)


def on_diagonal():
    row = lax.broadcasted_iota(jnp.int32, (PANEL, PANEL), 0)
    return row == lax.broadcasted_iota(jnp.int32, (PANEL, PANEL), 1)


def fold(values):
    return jnp.sum((values * values).reshape(values.shape[0] // 8, 8, values.shape[1]), axis=0)


def damping_of(pick):
    value = jnp.float32(DAMPINGS[0])
    for index in range(1, len(DAMPINGS)):
        value = jnp.where(pick == index, jnp.float32(DAMPINGS[index]), value)
    return value


def put_symmetric(ref, start, tile):
    stop = start + PANEL
    ref[:stop, start:stop] = tile
    if start:
        ref[start:stop, :start] = tile[:start].T


def rows_of(values):
    return values.reshape(-1, values.shape[-1])


def precondition_block(act, grad, quartic, damping, gradient, current, factor, second, square, root):
    order = jnp.where(quartic == 1, 4.0, 2.0)
    inverse_order = jnp.where(quartic == 1, 0.25, 0.5)
    rounded = dot(act, grad, LEFT_T).astype(jnp.bfloat16)
    gradient[...] = rounded
    trace = jnp.sum(fold(rounded.astype(jnp.float32)))
    shift = damping * (trace / BLK + 1.0)
    scale = BLK / (2.0 * (trace + BLK * shift))

    for side, dims in ((0, RIGHT_T), (1, LEFT_T)):
        for start in range(0, BLK, PANEL):
            stop = start + PANEL
            if side == 0:
                tile = dot(gradient[:stop, :], gradient[start:stop, :], dims)
            else:
                tile = dot(gradient[:, :stop], gradient[:, start:stop], dims)
            value = (tile[start:] + jnp.where(on_diagonal(), shift, 0.0)) * scale
            corner = (jnp.where(on_diagonal(), order + 1.0, 0.0) - value) * inverse_order
            if start:
                above = tile[:start] * scale
                value = jnp.concatenate([above, value], axis=0)
                corner = jnp.concatenate([-above * inverse_order, corner], axis=0)
            put_symmetric(current.at[side], start, value.astype(jnp.bfloat16))
            put_symmetric(factor.at[side], start, corner.astype(jnp.bfloat16))

    @pl.loop(0, 2)
    def _(side):
        for start in range(0, BLK, PANEL):
            stop = start + PANEL
            tile = dot(factor[side, :stop, :], factor[side, :, start:stop])
            put_symmetric(square.at[0], start, tile.astype(jnp.bfloat16))
        for start in range(0, BLK, PANEL):
            stop = start + PANEL
            tile = dot(square[0, :stop, :], square[0, :, start:stop]).astype(jnp.bfloat16)
            tile = jnp.where(quartic == 1, tile, square[0, :stop, start:stop])
            put_symmetric(square.at[1], start, tile)
        for start in range(0, BLK, PANEL):
            stop = start + PANEL
            tile = dot(square[1], current[side, :, start:stop])
            column = lax.broadcasted_iota(jnp.int32, (BLK, PANEL), 1) + start
            diagonal = lax.broadcasted_iota(jnp.int32, (BLK, PANEL), 0) == column
            tile = (jnp.where(diagonal, order + 1.0, 0.0) - tile) * inverse_order
            second[:, start:stop] = tile.astype(jnp.bfloat16)
        root[side] = dot(factor[side], second[...]).astype(jnp.bfloat16)


def gather_kernel(
    sizes, act, grad, table, exponents, picks, assembled, all_roots, sums,
    acts, grads, gradient, current, factor, second, square, root, update,
    total, own_sum, other_sum,
    load_sem, z_send, z_recv, y_send, y_recv, d_send, d_recv, root_sem, update_sem, s_send, s_recv,
):
    owners, row_blocks, col_blocks = sizes
    planes = owners // 2
    me = lax.axis_index("dp")
    core = lax.axis_index("mp")
    plane, lane = me // 2, lax.rem(me, 2)
    beside = {"dp": me + 1 - 2 * lane}
    other_core = {"mp": 1 - core}

    def source(offset):
        return lax.rem(plane + planes - offset, planes) * 2

    barrier = pltpu.get_barrier_semaphore()
    for offset in range(1, planes):
        target = {"dp": lax.rem(plane + offset, planes) * 2 + lane}
        pl.semaphore_signal(barrier, inc=1, device_id=target, device_id_type=MESH)
    pl.semaphore_signal(barrier, inc=1, device_id=beside, device_id_type=MESH)
    pl.semaphore_signal(barrier, inc=1, device_id=other_core, device_id_type=MESH)

    def place(unit, index):
        if unit < row_blocks:
            return acts.at[unit, index, core]
        return grads.at[unit - row_blocks, index]

    def column_place(col, index):
        return grads.at[col, index]

    def remote(ref, send, recv, target):
        return pltpu.make_async_remote_copy(
            src_ref=ref, dst_ref=ref, send_sem=send, recv_sem=recv,
            device_id=target, device_id_type=MESH,
        )

    def along(unit, ref_of, offset):
        target = {"dp": lax.rem(plane + offset, planes) * 2 + lane}
        return remote(ref_of(me), z_send.at[unit, offset], z_recv.at[unit, offset], target)

    def arriving_along(unit, ref_of, offset):
        ref = ref_of(source(offset) + lane)
        return remote(ref, z_send.at[unit, offset], z_recv.at[unit, offset], beside)

    def across(unit, ref_of, offset):
        ref = ref_of(source(offset) + lane)
        return remote(ref, y_send.at[unit, offset], y_recv.at[unit, offset], beside)

    def arriving_across(unit, ref_of, offset):
        ref = ref_of(source(offset) + 1 - lane)
        return remote(ref, y_send.at[unit, offset], y_recv.at[unit, offset], beside)

    def send_own(unit, ref_of):
        for offset in range(1, planes):
            along(unit, ref_of, offset).start()
        across(unit, ref_of, 0).start()

    def pass_on(unit, ref_of, offsets):
        for offset in offsets:
            arriving_along(unit, ref_of, offset).wait_recv()
            across(unit, ref_of, offset).start()

    def finish(unit, ref_of):
        for offset in range(planes):
            arriving_across(unit, ref_of, offset).wait_recv()

    def over(row):
        return remote(acts.at[row, :, core], d_send.at[row], d_recv.at[row], other_core)

    def arriving_over(row):
        return remote(acts.at[row, :, 1 - core], d_send.at[row], d_recv.at[row], other_core)

    def load_act(row):
        return pltpu.make_async_copy(
            act.at[core, :, pl.ds(row * BLK, BLK)], acts.at[row, me, core], load_sem.at[row]
        )

    def load_grad(col):
        return pltpu.make_async_copy(
            grad.at[:, pl.ds(col * BLK, BLK)], grads.at[col, me], load_sem.at[row_blocks + col]
        )

    for row in range(row_blocks):
        load_act(row).start()
    for col in range(col_blocks):
        load_grad(col).start()
    pl.semaphore_wait(barrier, planes + 1)
    early = row_blocks + min(2, col_blocks)
    for unit in range(row_blocks + col_blocks):
        if unit < row_blocks:
            load_act(unit).wait()
        else:
            load_grad(unit - row_blocks).wait()
        if unit < early:
            send_own(unit, functools.partial(place, unit))
    for row in range(row_blocks):
        pass_on(row, functools.partial(place, row), range(1, planes))
        finish(row, functools.partial(place, row))
        over(row).start()
    pass_on(row_blocks, functools.partial(place, row_blocks), range(1, planes))
    if col_blocks > 2:
        send_own(row_blocks + 2, functools.partial(place, row_blocks + 2))
    finish(row_blocks, functools.partial(place, row_blocks))
    for row in range(row_blocks):
        arriving_over(row).wait_recv()

    total[...] = jnp.zeros_like(total)

    def write_roots(block_id):
        return pltpu.make_async_copy(root, all_roots.at[block_id], root_sem)

    def write_update(row, col):
        to = assembled.at[pl.ds(row * BLK, BLK), pl.ds(col * BLK, BLK)]
        return pltpu.make_async_copy(update, to, update_sem)

    @pl.loop(0, row_blocks * col_blocks)
    def _(step):
        col = step // row_blocks
        row = lax.rem(step, row_blocks)
        following = row_blocks + col + 1
        block_id = row * col_blocks + col
        slot = table[0, block_id]

        @pl.when(jnp.logical_and(row == 0, step > 0))
        def _():
            finish(row_blocks + col, functools.partial(column_place, col))

        @pl.when(step > 0)
        def _():
            write_roots(block_id).wait()

        @pl.when(jnp.logical_and(row == row_blocks - 1, col + 1 < col_blocks))
        def _():
            pass_on(following, functools.partial(column_place, col + 1), range(1, planes))

        @pl.when(jnp.logical_and(row == row_blocks - 1, col + 3 < col_blocks))
        def _():
            send_own(following + 2, functools.partial(column_place, col + 3))

        precondition_block(
            rows_of(acts[row]), rows_of(grads[col]), exponents[0, slot], damping_of(picks[0, slot]),
            gradient, current, factor, second, square, root,
        )
        write_roots(block_id).start()
        second[...] = dot(root[0], gradient[...]).astype(jnp.bfloat16)
        rounded = dot(second[...], root[1]).astype(jnp.bfloat16)

        @pl.when(step > 0)
        def _():
            write_update(row, col).wait()

        update[...] = rounded
        total[...] += fold(rounded.astype(jnp.float32))
        write_update(row, col).start()

    lanes = total[:, :128]
    for start in range(128, BLK, 128):
        lanes = lanes + total[:, start : start + 128]
    own_sum[...] = lanes
    exchange = pltpu.make_async_remote_copy(
        src_ref=own_sum, dst_ref=other_sum, send_sem=s_send, recv_sem=s_recv,
        device_id=other_core, device_id_type=MESH,
    )
    exchange.start()
    write_roots(0).wait()
    write_update(0, 0).wait()
    for unit in range(row_blocks + col_blocks):
        for offset in range(1, planes):
            along(unit, functools.partial(place, unit), offset).wait_send()
        for offset in range(planes):
            across(unit, functools.partial(place, unit), offset).wait_send()
    for row in range(row_blocks):
        over(row).wait_send()
    exchange.wait()
    sums[...] = own_sum[...] + other_sum[...]


def gathered_updates(act, grad, table, exponents, picks, owners, halves):
    tokens, width = act.shape
    half_width = grad.shape[1]
    row_blocks, col_blocks = width // BLK, half_width // BLK
    blocks, units = row_blocks * col_blocks, row_blocks + col_blocks
    planes = owners // 2
    one = pltpu.VMEM((BLK, BLK), jnp.bfloat16)
    two = pltpu.VMEM((2, BLK, BLK), jnp.bfloat16)
    small = pltpu.VMEM((8, 128), jnp.float32)
    dma = pltpu.SemaphoreType.DMA
    hbm = pl.BlockSpec(memory_space=pl.ANY)
    smem = pl.BlockSpec(memory_space=pltpu.SMEM)
    return pl.pallas_call(
        functools.partial(gather_kernel, (owners, row_blocks, col_blocks)),
        out_shape=(
            jax.ShapeDtypeStruct((row_blocks * BLK, half_width), jnp.bfloat16),
            jax.ShapeDtypeStruct((blocks, 2, BLK, BLK), jnp.bfloat16),
            jax.ShapeDtypeStruct((8, 128), jnp.float32),
        ),
        in_specs=[hbm, hbm, smem, smem, smem],
        out_specs=(hbm, hbm, pl.BlockSpec(memory_space=pltpu.VMEM)),
        scratch_shapes=[
            pltpu.VMEM((row_blocks, owners, halves, tokens // halves, BLK), jnp.bfloat16),
            pltpu.VMEM((col_blocks, owners, tokens, BLK), jnp.bfloat16),
            one, two, two, one, two, two, one,
            pltpu.VMEM((8, BLK), jnp.float32), small, small,
            dma((units,)), dma((units, planes)), dma((units, planes)),
            dma((units, planes)), dma((units, planes)),
            dma((row_blocks,)), dma((row_blocks,)),
            dma, dma, dma, dma,
        ],
        compiler_params=pltpu.CompilerParams(
            collective_id=0, has_side_effects=True, vmem_limit_bytes=VMEM_BYTES
        ),
        cost_estimate=pl.CostEstimate(
            flops=blocks * 26 * BLK**3, bytes_accessed=blocks * 6 * BLK**2, transcendentals=0
        ),
        name="gathered_updates",
    )(act.reshape(halves, tokens // halves, width), grad, table, exponents, picks)


def empty_root(quartic, damping):
    def narrow(value):
        return value.astype(jnp.bfloat16).astype(jnp.float32)

    ones = jnp.ones((8, 128), jnp.float32)
    order = jnp.where(quartic == 1, 4.0, 2.0)
    inverse_order = jnp.where(quartic == 1, 0.25, 0.5)
    start = ones * (damping * (BLK / (2.0 * (BLK * damping))))
    factor = narrow((order + 1.0 - start) * inverse_order)
    square = narrow(factor * factor)
    raised = jnp.where(quartic == 1, narrow(square * square), square)
    second = narrow((order + 1.0 - raised * narrow(start)) * inverse_order)
    return (factor * second)[:1, :1]


def finish_kernel(steps, per_owner, count, ints, exponents, picks, sums, unscaled, roots_in, out, roots_out):
    index = pl.program_id(0)
    total = jnp.sum(sums[...])
    rescale = lax.rsqrt(jnp.full((1, 128), total / count + 1.0, jnp.float32))[:1, :1]
    out[...] = (unscaled[...].astype(jnp.float32) * rescale).astype(jnp.bfloat16)
    each = steps // per_owner
    which = index // each
    slot = ints[per_owner] * per_owner + which
    filled = ints[which] > 0

    @pl.when(filled)
    def _():
        roots_out[...] = roots_in[...]

    @pl.when(jnp.logical_not(filled))
    def _():
        value = empty_root(exponents[slot], damping_of(picks[slot]))
        rows = roots_out.shape[2]
        first = lax.rem(lax.rem(index, each) * rows, BLK)
        row = lax.broadcasted_iota(jnp.int32, (rows, BLK), 0) + first
        diagonal = row == lax.broadcasted_iota(jnp.int32, (rows, BLK), 1)
        roots_out[0, 0] = jnp.where(diagonal, value, 0.0).astype(jnp.bfloat16)


def finish(ints, exponents, picks, sums, unscaled, all_roots, per_owner, count):
    height, width = unscaled.shape
    each = 4 if per_owner > 1 else 8
    steps = each * per_owner
    rows = 2 * BLK // each
    parts = BLK // rows

    def own(i, ints, e, p):
        block_id = jnp.maximum(ints[i // each] - 1, 0)
        within = lax.rem(i, each)
        return block_id, within // parts, lax.rem(within, parts), 0

    def placed(i, ints, e, p):
        within = lax.rem(i, each)
        return i // each, within // parts, lax.rem(within, parts), 0

    return pl.pallas_call(
        functools.partial(finish_kernel, steps, per_owner, count),
        out_shape=(
            jax.ShapeDtypeStruct((height, width), jnp.bfloat16),
            jax.ShapeDtypeStruct((per_owner, 2, BLK, BLK), jnp.bfloat16),
        ),
        grid_spec=pltpu.PrefetchScalarGridSpec(
            num_scalar_prefetch=3,
            grid=(steps,),
            in_specs=[
                pl.BlockSpec((8, 128), lambda i, a, e, p: (0, 0)),
                pl.BlockSpec((height // steps, width), lambda i, a, e, p: (i, 0)),
                pl.BlockSpec((1, 1, rows, BLK), own),
            ],
            out_specs=(
                pl.BlockSpec((height // steps, width), lambda i, a, e, p: (i, 0)),
                pl.BlockSpec((1, 1, rows, BLK), placed),
            ),
        ),
        compiler_params=pltpu.CompilerParams(vmem_limit_bytes=40 * 1024 * 1024),
        cost_estimate=pl.CostEstimate(
            flops=10**9, bytes_accessed=4 * height * width, transcendentals=0
        ),
        name="scaled_update",
    )(ints, exponents, picks, sums, unscaled, all_roots)


def on_device(activations, out_grads, slot_table, exponent_index, damping_index):
    half_width = out_grads.shape[1]
    half_blocks = (activations.shape[1] // BLK) * (half_width // BLK)
    owners = lax.axis_size("dp")
    halves = lax.axis_size("mp")
    per_owner = slot_table.shape[1] // owners
    me = lax.axis_index("dp")

    places = jnp.arange(per_owner + 1, dtype=jnp.int32)
    matches = slot_table[0, :half_blocks][None, :] == (me * per_owner + places)[:, None]
    held = jnp.sum(jnp.where(matches, jnp.arange(1, half_blocks + 1, dtype=jnp.int32)[None, :], 0), axis=1)
    ints = jnp.where(places == per_owner, me, held).astype(jnp.int32)

    assembled, all_roots, sums = gathered_updates(
        activations, out_grads, slot_table, exponent_index, damping_index, owners, halves
    )
    count = float(activations.shape[1] * half_width * halves)
    update, roots = finish(
        ints, exponent_index[0], damping_index[0], sums, assembled, all_roots, per_owner, count
    )
    return (update, roots[None])


def solution(mesh):
    placed = (
        P(("member", "dp"), None),
        P(("member", "dp"), "mp"),
        P(("member", "mp"), None),
        P(("member", "mp"), None),
        P(("member", "mp"), None),
    )
    return jax.shard_map(
        on_device,
        mesh=mesh,
        in_specs=placed,
        out_specs=(P("member", "mp"), P(("member", "mp"), "dp", None, None, None)),
        check_vma=False,
    )
```

```python
import functools

import jax
import jax.numpy as jnp
from jax import lax
from jax.experimental import pallas as pl
from jax.experimental.pallas import tpu as pltpu
from jax.sharding import PartitionSpec as P

BLK = 1024
PANEL = 256
DAMPINGS = (0.03, 0.1, 0.3, 1.0)
VMEM_BYTES = 60 * 1024 * 1024
RESIDENT_BYTES = 60 * 1024 * 1024
RESIDENT_LIMIT = 43 * 1024 * 1024

NORMAL = (((1,), (0,)), ((), ()))
LEFT_T = (((0,), (0,)), ((), ()))
RIGHT_T = (((1,), (1,)), ((), ()))
MESH = pl.DeviceIdType.MESH


def dot(lhs, rhs, dims=NORMAL):
    return lax.dot_general(lhs, rhs, dims, preferred_element_type=jnp.float32)


def on_diagonal():
    row = lax.broadcasted_iota(jnp.int32, (PANEL, PANEL), 0)
    return row == lax.broadcasted_iota(jnp.int32, (PANEL, PANEL), 1)


def fold(values):
    return jnp.sum((values * values).reshape(values.shape[0] // 8, 8, values.shape[1]), axis=0)


def damping_of(pick):
    value = jnp.float32(DAMPINGS[0])
    for index in range(1, len(DAMPINGS)):
        value = jnp.where(pick == index, jnp.float32(DAMPINGS[index]), value)
    return value


def put_symmetric(ref, start, tile):
    stop = start + PANEL
    ref[:stop, start:stop] = tile
    if start:
        ref[start:stop, :start] = tile[:start].T


def rows_of(values):
    return values.reshape(-1, values.shape[-1])


def precondition_block(
    act, grad, quartic, damping, gradient, current, factor, second, square, root, between=None
):
    order = jnp.where(quartic == 1, 4.0, 2.0)
    inverse_order = jnp.where(quartic == 1, 0.25, 0.5)
    rounded = dot(act, grad, LEFT_T).astype(jnp.bfloat16)
    gradient[...] = rounded
    trace = jnp.sum(fold(rounded.astype(jnp.float32)))
    shift = damping * (trace / BLK + 1.0)
    scale = BLK / (2.0 * (trace + BLK * shift))

    @pl.loop(0, 2)
    def _(side):
        def statistic(tile_of):
            for start in range(0, BLK, PANEL):
                tile = tile_of(start, start + PANEL)
                value = (tile[start:] + jnp.where(on_diagonal(), shift, 0.0)) * scale
                corner = (jnp.where(on_diagonal(), order + 1.0, 0.0) - value) * inverse_order
                if start:
                    above = tile[:start] * scale
                    value = jnp.concatenate([above, value], axis=0)
                    corner = jnp.concatenate([-above * inverse_order, corner], axis=0)
                put_symmetric(current, start, value.astype(jnp.bfloat16))
                put_symmetric(factor, start, corner.astype(jnp.bfloat16))

        @pl.when(side == 0)
        def _():
            statistic(lambda start, stop: dot(gradient[:stop, :], gradient[start:stop, :], RIGHT_T))

        @pl.when(side == 1)
        def _():
            statistic(lambda start, stop: dot(gradient[:, :stop], gradient[:, start:stop], LEFT_T))

        if between is not None:
            between(side)

        for start in range(0, BLK, PANEL):
            stop = start + PANEL
            tile = dot(factor[:stop, :], factor[:, start:stop])
            put_symmetric(square.at[0], start, tile.astype(jnp.bfloat16))
        for start in range(0, BLK, PANEL):
            stop = start + PANEL
            tile = dot(square[0, :stop, :], square[0, :, start:stop]).astype(jnp.bfloat16)
            tile = jnp.where(quartic == 1, tile, square[0, :stop, start:stop])
            put_symmetric(square.at[1], start, tile)
        for start in range(0, BLK, PANEL):
            stop = start + PANEL
            tile = dot(square[1], current[:, start:stop])
            column = lax.broadcasted_iota(jnp.int32, (BLK, PANEL), 1) + start
            diagonal = lax.broadcasted_iota(jnp.int32, (BLK, PANEL), 0) == column
            tile = (jnp.where(diagonal, order + 1.0, 0.0) - tile) * inverse_order
            second[:, start:stop] = tile.astype(jnp.bfloat16)
        root[side] = dot(factor[...], second[...]).astype(jnp.bfloat16)


def gather_kernel(plan, *refs):
    owners, row_blocks, col_blocks, resident, trade = plan
    act, grad, table, exponents, picks, assembled, all_roots, sums = refs[:8]
    refs = refs[8:]
    if trade:
        kept_acts, kept_grads, kept_sem, trade_send, trade_recv = refs[0], refs[1], *refs[-3:]
        refs = refs[2:-3]
    acts, grads, gradient, current, factor, second, square, root, total, own_sum, other_sum = refs[:11]
    refs = refs[11:]
    if not resident:
        update, update_sem = refs[0], refs[-1]
        refs = refs[1:-1]
    load_sem, z_send, z_recv, y_send, y_recv, d_send, d_recv, root_sem, s_send, s_recv = refs

    planes = owners // 2
    me = lax.axis_index("dp")
    core = lax.axis_index("mp")
    plane, lane = me // 2, lax.rem(me, 2)
    parity = lax.rem(plane, 2)
    beside = {"dp": me + 1 - 2 * lane}
    facing = {"dp": me + 2 - 4 * parity}
    other_core = {"mp": 1 - core}
    y_col, z_col = col_blocks - 3, col_blocks - 2

    def source(offset):
        return lax.rem(plane + planes - offset, planes) * 2

    barrier = pltpu.get_barrier_semaphore()
    for offset in range(1, planes):
        target = {"dp": lax.rem(plane + offset, planes) * 2 + lane}
        pl.semaphore_signal(barrier, inc=1, device_id=target, device_id_type=MESH)
    pl.semaphore_signal(barrier, inc=1, device_id=beside, device_id_type=MESH)
    pl.semaphore_signal(barrier, inc=1, device_id=other_core, device_id_type=MESH)

    def act_place(row):
        return row, lambda index: acts.at[row, index, core]

    def grad_place(col):
        return row_blocks + col, lambda index: grads.at[col, index]

    def remote(ref, send, recv, target):
        return pltpu.make_async_remote_copy(
            src_ref=ref, dst_ref=ref, send_sem=send, recv_sem=recv,
            device_id=target, device_id_type=MESH,
        )

    def along(place, offset):
        unit, ref_of = place
        target = {"dp": lax.rem(plane + offset, planes) * 2 + lane}
        return remote(ref_of(me), z_send.at[unit, offset], z_recv.at[unit, offset], target)

    def arriving_along(place, offset):
        unit, ref_of = place
        ref = ref_of(source(offset) + lane)
        return remote(ref, z_send.at[unit, offset], z_recv.at[unit, offset], beside)

    def across(place, offset):
        unit, ref_of = place
        ref = ref_of(source(offset) + lane)
        return remote(ref, y_send.at[unit, offset], y_recv.at[unit, offset], beside)

    def arriving_across(place, offset):
        unit, ref_of = place
        ref = ref_of(source(offset) + 1 - lane)
        return remote(ref, y_send.at[unit, offset], y_recv.at[unit, offset], beside)

    def send_own(place):
        for offset in range(1, planes):
            along(place, offset).start()
        across(place, 0).start()

    def pass_on(place):
        for offset in range(1, planes):
            arriving_along(place, offset).wait_recv()
            across(place, offset).start()

    def finish(place):
        for offset in range(planes):
            arriving_across(place, offset).wait_recv()

    def over(row):
        return remote(acts.at[row, :, core], d_send.at[row], d_recv.at[row], other_core)

    def arriving_over(row):
        return remote(acts.at[row, :, 1 - core], d_send.at[row], d_recv.at[row], other_core)

    def load_act(row):
        return pltpu.make_async_copy(
            act.at[core, :, pl.ds(row * BLK, BLK)], acts.at[row, me, core], load_sem.at[row]
        )

    def load_grad(col):
        return pltpu.make_async_copy(
            grad.at[:, pl.ds(col * BLK, BLK)], grads.at[col, me], load_sem.at[row_blocks + col]
        )

    load_act(0).start()
    load_grad(0).start()
    for row in range(1, row_blocks):
        load_act(row).start()
    for col in range(1, col_blocks):
        load_grad(col).start()
    pl.semaphore_wait(barrier, planes + 1)
    load_act(0).wait()
    send_own(act_place(0))
    load_grad(0).wait()
    send_own(grad_place(0))
    for row in range(1, row_blocks):
        load_act(row).wait()
    for col in range(1, col_blocks):
        load_grad(col).wait()
    pass_on(act_place(0))
    pass_on(grad_place(0))
    for row in range(1, row_blocks):
        send_own(act_place(row))
    finish(act_place(0))
    over(0).start()
    finish(grad_place(0))
    arriving_over(0).wait_recv()
    total[...] = jnp.zeros_like(total)

    def write_roots(block_id):
        return pltpu.make_async_copy(root, all_roots.at[block_id], root_sem)

    def write_update(block_id):
        return pltpu.make_async_copy(update, assembled.at[block_id], update_sem)

    def keep_act(row):
        return pltpu.make_async_copy(acts.at[row], kept_acts.at[row], kept_sem.at[row])

    def keep_grad(index):
        return pltpu.make_async_copy(
            grads.at[y_col + index], kept_grads.at[index], kept_sem.at[row_blocks + index]
        )

    def traded(index, theirs):
        row = (lane, parity)[index]
        row = 1 - row if theirs else row
        block_id = row * col_blocks + y_col + index
        return block_id, remote(
            assembled.at[block_id], trade_send.at[index], trade_recv.at[index], (beside, facing)[index]
        )

    steps = row_blocks * col_blocks - (2 if trade else 0)

    @pl.loop(0, steps)
    def _(step):
        col = step // row_blocks
        row = lax.rem(step, row_blocks)
        begins = row == 0
        if trade:
            both = row_blocks * y_col
            last = jnp.logical_and(step >= both + 2, True)
            row = jnp.where(step == both, lane, jnp.where(step == both + 1, parity, row))
            col = jnp.where(step < both, col, jnp.where(last, col_blocks - 1, y_col + step - both))
            begins = jnp.logical_or(begins, step == both + 1)
        block_id = row * col_blocks + col
        slot = table[0, block_id]

        @pl.when(jnp.logical_and(begins, step > 0))
        def _():
            finish(grad_place(col))

        for other in range(1, row_blocks):
            @pl.when(step == other)
            def _():
                arriving_over(other).wait_recv()

        @pl.when(step > 0)
        def _():
            write_roots(block_id).wait()

        def between(side):
            @pl.when(jnp.logical_and(side == 0, step == 0))
            def _():
                for other in range(1, row_blocks):
                    pass_on(act_place(other))
                send_own(grad_place(1))

            @pl.when(jnp.logical_and(side == 0, jnp.logical_and(step > 0, step < col_blocks)))
            def _():
                pass_on(grad_place(step))

            @pl.when(jnp.logical_and(side == 0, jnp.logical_and(step > 0, step + 1 < col_blocks)))
            def _():
                send_own(grad_place(step + 1))

        precondition_block(
            rows_of(acts[row]), rows_of(grads[col]), exponents[0, slot], damping_of(picks[0, slot]),
            gradient, current, factor, second, square, root, between,
        )

        @pl.when(step == 0)
        def _():
            for other in range(1, row_blocks):
                finish(act_place(other))
                over(other).start()

        write_roots(block_id).start()
        second[...] = dot(root[0], gradient[...]).astype(jnp.bfloat16)
        rounded = dot(second[...], root[1]).astype(jnp.bfloat16)
        total[...] += fold(rounded.astype(jnp.float32))
        if resident:
            assembled[block_id] = rounded
        else:
            @pl.when(step > 0)
            def _():
                write_update(block_id).wait()

            update[...] = rounded
            write_update(block_id).start()
        if trade:
            for index in range(2):
                @pl.when(step == both + index)
                def _():
                    traded(index, False)[1].start()
                    keep_act(index).start()
                    keep_grad(index).start()

    if trade:
        for index in range(2):
            block_id, copy = traded(index, True)
            copy.wait_recv()
            total[...] += fold(assembled[block_id].astype(jnp.float32))
    lanes = total[:, :128]
    for start in range(128, BLK, 128):
        lanes = lanes + total[:, start : start + 128]
    own_sum[...] = lanes
    exchange = pltpu.make_async_remote_copy(
        src_ref=own_sum, dst_ref=other_sum, send_sem=s_send, recv_sem=s_recv,
        device_id=other_core, device_id_type=MESH,
    )
    exchange.start()
    write_roots(0).wait()
    if not resident:
        write_update(0).wait()
    if trade:
        for index in range(2):
            traded(index, False)[1].wait_send()
            keep_act(index).wait()
            keep_grad(index).wait()
    for place in [act_place(row) for row in range(row_blocks)] + [grad_place(col) for col in range(col_blocks)]:
        for offset in range(1, planes):
            along(place, offset).wait_send()
        for offset in range(planes):
            across(place, offset).wait_send()
    for row in range(row_blocks):
        over(row).wait_send()
    exchange.wait()
    sums[...] = own_sum[...] + other_sum[...]


def gathered_updates(act, grad, table, exponents, picks, plan, halves):
    owners, row_blocks, col_blocks, resident, trade = plan
    tokens, width = act.shape
    blocks, units = row_blocks * col_blocks, row_blocks + col_blocks
    planes = owners // 2
    one = pltpu.VMEM((BLK, BLK), jnp.bfloat16)
    two = pltpu.VMEM((2, BLK, BLK), jnp.bfloat16)
    small = pltpu.VMEM((8, 128), jnp.float32)
    dma = pltpu.SemaphoreType.DMA
    hbm = pl.BlockSpec(memory_space=pl.ANY)
    smem = pl.BlockSpec(memory_space=pltpu.SMEM)
    vmem = pl.BlockSpec(memory_space=pltpu.VMEM)
    acts_shape = (row_blocks, owners, halves, tokens // halves, BLK)
    grads_shape = (col_blocks, owners, tokens, BLK)
    shapes = [
        (pltpu.VMEM if resident else pltpu.HBM)((blocks, BLK, BLK), jnp.bfloat16),
        pltpu.HBM((blocks, 2, BLK, BLK), jnp.bfloat16),
        jax.ShapeDtypeStruct((8, 128), jnp.float32),
    ]
    specs = [vmem if resident else hbm, hbm, vmem]
    if trade:
        shapes += [
            pltpu.HBM(acts_shape, jnp.bfloat16),
            pltpu.HBM((2,) + grads_shape[1:], jnp.bfloat16),
        ]
        specs += [hbm, hbm]
    scratch = [
        pltpu.VMEM(acts_shape, jnp.bfloat16), pltpu.VMEM(grads_shape, jnp.bfloat16),
        one, one, one, one, two, two, pltpu.VMEM((8, BLK), jnp.float32), small, small,
    ]
    sems = [
        dma((units,)), dma((units, planes)), dma((units, planes)),
        dma((units, planes)), dma((units, planes)), dma((row_blocks,)), dma((row_blocks,)),
        dma, dma, dma,
    ]
    if not resident:
        scratch, sems = scratch + [one], sems + [dma]
    if trade:
        sems += [dma((row_blocks + 2,)), dma((2,)), dma((2,))]
    return pl.pallas_call(
        functools.partial(gather_kernel, plan),
        out_shape=tuple(shapes),
        in_specs=[hbm, hbm, smem, smem, smem],
        out_specs=tuple(specs),
        scratch_shapes=scratch + sems,
        compiler_params=pltpu.CompilerParams(
            collective_id=0, has_side_effects=True,
            vmem_limit_bytes=RESIDENT_LIMIT if resident else VMEM_BYTES,
        ),
        cost_estimate=pl.CostEstimate(
            flops=blocks * 26 * BLK**3, bytes_accessed=blocks * 6 * BLK**2, transcendentals=0
        ),
        name="gathered_updates",
    )(act.reshape(halves, tokens // halves, width), grad, table, exponents, picks)


def empty_root(quartic, damping):
    def narrow(value):
        return value.astype(jnp.bfloat16).astype(jnp.float32)

    ones = jnp.ones((8, 128), jnp.float32)
    order = jnp.where(quartic == 1, 4.0, 2.0)
    inverse_order = jnp.where(quartic == 1, 0.25, 0.5)
    start = ones * (damping * (BLK / (2.0 * (BLK * damping))))
    factor = narrow((order + 1.0 - start) * inverse_order)
    square = narrow(factor * factor)
    raised = jnp.where(quartic == 1, narrow(square * square), square)
    second = narrow((order + 1.0 - raised * narrow(start)) * inverse_order)
    return (factor * second)[:1, :1]


def finish_kernel(plan, per_owner, count, *refs):
    owners, row_blocks, col_blocks, resident, trade = plan
    ints, exponents, picks, sums, unscaled, all_roots = refs[:6]
    refs = refs[6:]
    if trade:
        kept_acts, kept_grads = refs[:2]
        refs = refs[2:]
    out, roots_out, stage, roots, stage_sem, root_load, root_store = refs[:7]
    if not resident:
        piece, piece_sem = refs[7:]
    if trade:
        act, grad, gradient, current, factor, second, square, kept_sem = refs[7:]
    blocks = row_blocks * col_blocks
    depth, rows = stage.shape[0], stage.shape[1]
    parts = BLK // rows
    me = ints[per_owner]
    plane, lane = me // 2, lax.rem(me, 2)
    parity = lax.rem(plane, 2)
    rescale = lax.rsqrt(jnp.full((8, 128), jnp.sum(sums[...]) / count + 1.0, jnp.float32))[:1, :1]

    def block_of(which):
        return jnp.maximum(ints[which] - 1, 0)

    def missing(which):
        if not trade:
            return jnp.bool_(False)
        block_id = block_of(which)
        first = (1 - lane) * col_blocks + col_blocks - 3
        second_id = (1 - parity) * col_blocks + col_blocks - 2
        hit = jnp.logical_or(block_id == first, block_id == second_id)
        return jnp.logical_and(hit, ints[which] > 0)

    def ready(which):
        return jnp.logical_and(ints[which] > 0, jnp.logical_not(missing(which)))

    def load_roots(which):
        return pltpu.make_async_copy(all_roots.at[block_of(which)], roots.at[which], root_load.at[which])

    def store_roots(which):
        return pltpu.make_async_copy(roots.at[which], roots_out.at[which], root_store.at[which])

    def store_piece(index, slot):
        block_id = index // parts
        at_row = (block_id // col_blocks) * BLK + lax.rem(index, parts) * rows
        at_col = lax.rem(block_id, col_blocks) * BLK
        to = out.at[pl.ds(pl.multiple_of(at_row, rows), rows), pl.ds(pl.multiple_of(at_col, BLK), BLK)]
        return pltpu.make_async_copy(stage.at[slot], to, stage_sem.at[slot])

    for which in range(per_owner):
        @pl.when(ready(which))
        def _():
            load_roots(which).start()

    def scale_pieces(first, stop):
        @pl.loop(first, stop)
        def _(index):
            slot = lax.rem(index, depth)

            @pl.when(index >= depth)
            def _():
                store_piece(index, slot).wait()

            at = pl.ds(pl.multiple_of(lax.rem(index, parts) * rows, rows), rows)
            if resident:
                values = unscaled[index // parts, at]
            else:
                load = pltpu.make_async_copy(unscaled.at[index // parts, at], piece, piece_sem)
                load.start()
                load.wait()
                values = piece[...]
            stage[slot] = (values.astype(jnp.float32) * rescale).astype(jnp.bfloat16)
            store_piece(index, slot).start()

    pieces = blocks * parts
    middle = max(depth, pieces // 2)
    scale_pieces(0, middle)
    for which in range(per_owner):
        @pl.when(ready(which))
        def _():
            load_roots(which).wait()
            store_roots(which).start()

        @pl.when(ints[which] == 0)
        def _():
            slot = me * per_owner + which
            value = empty_root(exponents[slot], damping_of(picks[slot]))
            for start in range(0, BLK, PANEL):
                row = lax.broadcasted_iota(jnp.int32, (PANEL, BLK), 0) + start
                diagonal = row == lax.broadcasted_iota(jnp.int32, (PANEL, BLK), 1)
                for side in range(2):
                    roots[which, side, start : start + PANEL, :] = jnp.where(
                        diagonal, value, 0.0
                    ).astype(jnp.bfloat16)
            store_roots(which).start()

    scale_pieces(middle, pieces)
    if trade:
        @pl.loop(0, per_owner)
        def _(which):
            @pl.when(missing(which))
            def _():
                block_id = block_of(which)
                col = lax.rem(block_id, col_blocks)
                loads = [
                    pltpu.make_async_copy(kept_acts.at[block_id // col_blocks], act, kept_sem.at[0]),
                    pltpu.make_async_copy(kept_grads.at[col - (col_blocks - 3)], grad, kept_sem.at[1]),
                ]
                for load in loads:
                    load.start()
                for load in loads:
                    load.wait()
                slot = me * per_owner + which
                precondition_block(
                    rows_of(act[...]), rows_of(grad[...]), exponents[slot], damping_of(picks[slot]),
                    gradient, current, factor, second, square, roots.at[which],
                )
                store_roots(which).start()

    for slot in range(depth):
        store_piece(slot, slot).wait()
    for which in range(per_owner):
        store_roots(which).wait()


def finish(ints, exponents, picks, gathered, plan, per_owner, count):
    owners, row_blocks, col_blocks, resident, trade = plan
    unscaled, all_roots, sums = gathered[:3]
    if resident:
        unscaled = pltpu.with_memory_space_constraint(unscaled, pltpu.VMEM)
    one = pltpu.VMEM((BLK, BLK), jnp.bfloat16)
    two = pltpu.VMEM((2, BLK, BLK), jnp.bfloat16)
    dma = pltpu.SemaphoreType.DMA
    hbm = pl.BlockSpec(memory_space=pl.ANY)
    smem = pl.BlockSpec(memory_space=pltpu.SMEM)
    vmem = pl.BlockSpec(memory_space=pltpu.VMEM)
    depth, rows = 4, 256
    scratch = [
        pltpu.VMEM((depth, rows, BLK), jnp.bfloat16),
        pltpu.VMEM((per_owner, 2, BLK, BLK), jnp.bfloat16),
        dma((depth,)), dma((per_owner,)), dma((per_owner,)),
    ]
    if not resident:
        scratch += [pltpu.VMEM((rows, BLK), jnp.bfloat16), dma]
    if trade:
        kept_acts, kept_grads = gathered[3:]
        scratch += [
            pltpu.VMEM(kept_acts.shape[1:], jnp.bfloat16), pltpu.VMEM(kept_grads.shape[1:], jnp.bfloat16),
            one, one, one, one, two, dma((2,)),
        ]
    return pl.pallas_call(
        functools.partial(finish_kernel, plan, per_owner, count),
        out_shape=(
            jax.ShapeDtypeStruct((row_blocks * BLK, col_blocks * BLK), jnp.bfloat16),
            jax.ShapeDtypeStruct((per_owner, 2, BLK, BLK), jnp.bfloat16),
        ),
        in_specs=[smem, smem, smem, vmem, vmem if resident else hbm, hbm] + [hbm] * (len(gathered) - 3),
        out_specs=(hbm, hbm),
        scratch_shapes=scratch,
        compiler_params=pltpu.CompilerParams(vmem_limit_bytes=RESIDENT_LIMIT),
        cost_estimate=pl.CostEstimate(
            flops=10**9, bytes_accessed=4 * row_blocks * col_blocks * BLK**2, transcendentals=0
        ),
        name="scaled_update",
    )(ints, exponents, picks, sums, unscaled, all_roots, *gathered[3:])


def on_device(activations, out_grads, slot_table, exponent_index, damping_index):
    half_width = out_grads.shape[1]
    half_blocks = (activations.shape[1] // BLK) * (half_width // BLK)
    owners = lax.axis_size("dp")
    halves = lax.axis_size("mp")
    per_owner = slot_table.shape[1] // owners
    me = lax.axis_index("dp")

    places = jnp.arange(per_owner + 1, dtype=jnp.int32)
    matches = slot_table[0, :half_blocks][None, :] == (me * per_owner + places)[:, None]
    held = jnp.sum(jnp.where(matches, jnp.arange(1, half_blocks + 1, dtype=jnp.int32)[None, :], 0), axis=1)
    ints = jnp.where(places == per_owner, me, held).astype(jnp.int32)

    row_blocks, col_blocks = activations.shape[1] // BLK, half_width // BLK
    tokens = activations.shape[0] * owners
    inputs = 2 * tokens * (activations.shape[1] + half_width)
    resident = inputs + 2 * (half_blocks + 10) * BLK * BLK <= RESIDENT_BYTES
    trade = resident and row_blocks == 2 and col_blocks > 3 and owners % 4 == 0
    plan = (owners, row_blocks, col_blocks, resident, trade)
    gathered = gathered_updates(
        activations, out_grads, slot_table, exponent_index, damping_index, plan, halves
    )
    count = float(activations.shape[1] * half_width * halves)
    update, roots = finish(ints, exponent_index[0], damping_index[0], gathered, plan, per_owner, count)
    return (update, roots[None])


def solution(mesh):
    placed = (
        P(("member", "dp"), None),
        P(("member", "dp"), "mp"),
        P(("member", "mp"), None),
        P(("member", "mp"), None),
        P(("member", "mp"), None),
    )
    return jax.shard_map(
        on_device,
        mesh=mesh,
        in_specs=placed,
        out_specs=(P("member", "mp"), P(("member", "mp"), "dp", None, None, None)),
        check_vma=False,
    )
```

```python
import functools

import jax
import jax.numpy as jnp
from jax import lax
from jax.experimental import pallas as pl
from jax.experimental.pallas import tpu as pltpu
from jax.sharding import PartitionSpec as P

BLK = 1024
PANEL = 256
DAMPINGS = (0.03, 0.1, 0.3, 1.0)
VMEM_BYTES = 60 * 1024 * 1024
RESIDENT_BYTES = 60 * 1024 * 1024
RESIDENT_LIMIT = 43 * 1024 * 1024

NORMAL = (((1,), (0,)), ((), ()))
LEFT_T = (((0,), (0,)), ((), ()))
RIGHT_T = (((1,), (1,)), ((), ()))
MESH = pl.DeviceIdType.MESH


def dot(lhs, rhs, dims=NORMAL):
    return lax.dot_general(lhs, rhs, dims, preferred_element_type=jnp.float32)


def on_diagonal():
    row = lax.broadcasted_iota(jnp.int32, (PANEL, PANEL), 0)
    return row == lax.broadcasted_iota(jnp.int32, (PANEL, PANEL), 1)


def fold(values):
    return jnp.sum((values * values).reshape(values.shape[0] // 8, 8, values.shape[1]), axis=0)


def damping_of(pick):
    value = jnp.float32(DAMPINGS[0])
    for index in range(1, len(DAMPINGS)):
        value = jnp.where(pick == index, jnp.float32(DAMPINGS[index]), value)
    return value


def put_symmetric(ref, start, tile):
    stop = start + PANEL
    ref[:stop, start:stop] = tile
    if start:
        ref[start:stop, :start] = tile[:start].T


def swap_of(table, trade, me, col_blocks, per_owner):
    col, kind = trade
    plane, lane = me // 2, lax.rem(me, 2)
    if kind == "y":
        low, high = 2 * plane, 2 * plane + 1
    else:
        low = 2 * (plane - lax.rem(plane, 2)) + lane
        high = low + 2
    upper, lower = table[0, col] // per_owner, table[0, col_blocks + col] // per_owner
    return jnp.logical_or(upper == high, lower == low).astype(jnp.int32)


def trader_row(kind, me):
    return lax.rem(me, 2) if kind == "y" else lax.rem(me // 2, 2)


def pick(index, values):
    picked = values[0]
    for place in range(1, len(values)):
        picked = jnp.where(index == place, values[place], picked)
    return picked


def form_gradient(gradient, act, grad):
    gradient[...] = dot(rows_of(act), rows_of(grad), LEFT_T).astype(jnp.bfloat16)


def rows_of(values):
    return values.reshape(-1, values.shape[-1])


def precondition_block(
    form, quartic, damping, gradient, current, factor, second, square, root, between=None
):
    order = jnp.where(quartic == 1, 4.0, 2.0)
    inverse_order = jnp.where(quartic == 1, 0.25, 0.5)
    form()
    trace = jnp.sum(fold(gradient[...].astype(jnp.float32)))
    shift = damping * (trace / BLK + 1.0)
    scale = BLK / (2.0 * (trace + BLK * shift))

    @pl.loop(0, 2)
    def _(side):
        def statistic(tile_of):
            for start in range(0, BLK, PANEL):
                tile = tile_of(start, start + PANEL)
                value = (tile[start:] + jnp.where(on_diagonal(), shift, 0.0)) * scale
                corner = (jnp.where(on_diagonal(), order + 1.0, 0.0) - value) * inverse_order
                if start:
                    above = tile[:start] * scale
                    value = jnp.concatenate([above, value], axis=0)
                    corner = jnp.concatenate([-above * inverse_order, corner], axis=0)
                put_symmetric(current, start, value.astype(jnp.bfloat16))
                put_symmetric(factor, start, corner.astype(jnp.bfloat16))

        @pl.when(side == 0)
        def _():
            statistic(lambda start, stop: dot(gradient[:stop, :], gradient[start:stop, :], RIGHT_T))

        @pl.when(side == 1)
        def _():
            statistic(lambda start, stop: dot(gradient[:, :stop], gradient[:, start:stop], LEFT_T))

        if between is not None:
            between(side)

        for start in range(0, BLK, PANEL):
            stop = start + PANEL
            tile = dot(factor[:stop, :], factor[:, start:stop])
            put_symmetric(square.at[0], start, tile.astype(jnp.bfloat16))
        for start in range(0, BLK, PANEL):
            stop = start + PANEL
            tile = dot(square[0, :stop, :], square[0, :, start:stop]).astype(jnp.bfloat16)
            tile = jnp.where(quartic == 1, tile, square[0, :stop, start:stop])
            put_symmetric(square.at[1], start, tile)
        for start in range(0, BLK, PANEL):
            stop = start + PANEL
            tile = dot(square[1], current[:, start:stop])
            column = lax.broadcasted_iota(jnp.int32, (BLK, PANEL), 1) + start
            diagonal = lax.broadcasted_iota(jnp.int32, (BLK, PANEL), 0) == column
            tile = (jnp.where(diagonal, order + 1.0, 0.0) - tile) * inverse_order
            second[:, start:stop] = tile.astype(jnp.bfloat16)
        root[side] = dot(factor[...], second[...]).astype(jnp.bfloat16)


def gather_kernel(plan, *refs):
    owners, row_blocks, col_blocks, per_owner, resident, trades = plan
    act, grad, table, exponents, picks, assembled, all_roots, sums = refs[:8]
    refs = refs[8:]
    if trades:
        kept_acts, kept_grads, kept_sem, trade_send, trade_recv = refs[0], refs[1], *refs[-3:]
        refs = refs[2:-3]
    acts, grads, gradient, current, factor, second, square, root, total, own_sum, other_sum = refs[:11]
    refs = refs[11:]
    if not resident:
        update, update_sem = refs[0], refs[-1]
        refs = refs[1:-1]
    load_sem, z_send, z_recv, y_send, y_recv, d_send, d_recv, root_sem, s_send, s_recv = refs

    planes = owners // 2
    me = lax.axis_index("dp")
    core = lax.axis_index("mp")
    plane, lane = me // 2, lax.rem(me, 2)
    parity = lax.rem(plane, 2)
    beside = {"dp": me + 1 - 2 * lane}
    facing = {"dp": me + 2 - 4 * parity}
    other_core = {"mp": 1 - core}

    def source(offset):
        return lax.rem(plane + planes - offset, planes) * 2

    barrier = pltpu.get_barrier_semaphore()
    for offset in range(1, planes):
        target = {"dp": lax.rem(plane + offset, planes) * 2 + lane}
        pl.semaphore_signal(barrier, inc=1, device_id=target, device_id_type=MESH)
    pl.semaphore_signal(barrier, inc=1, device_id=beside, device_id_type=MESH)
    pl.semaphore_signal(barrier, inc=1, device_id=other_core, device_id_type=MESH)

    def act_place(row):
        return row, lambda index: acts.at[row, index, core]

    def grad_place(col):
        return row_blocks + col, lambda index: grads.at[col, index]

    def remote(ref, send, recv, target):
        return pltpu.make_async_remote_copy(
            src_ref=ref, dst_ref=ref, send_sem=send, recv_sem=recv,
            device_id=target, device_id_type=MESH,
        )

    def along(place, offset):
        unit, ref_of = place
        target = {"dp": lax.rem(plane + offset, planes) * 2 + lane}
        return remote(ref_of(me), z_send.at[unit, offset], z_recv.at[unit, offset], target)

    def arriving_along(place, offset):
        unit, ref_of = place
        ref = ref_of(source(offset) + lane)
        return remote(ref, z_send.at[unit, offset], z_recv.at[unit, offset], beside)

    def across(place, offset):
        unit, ref_of = place
        ref = ref_of(source(offset) + lane)
        return remote(ref, y_send.at[unit, offset], y_recv.at[unit, offset], beside)

    def arriving_across(place, offset):
        unit, ref_of = place
        ref = ref_of(source(offset) + 1 - lane)
        return remote(ref, y_send.at[unit, offset], y_recv.at[unit, offset], beside)

    def send_along(place):
        for offset in range(1, planes):
            along(place, offset).start()

    def send_across(place):
        across(place, 0).start()

    def pass_on(place):
        for offset in range(1, planes):
            arriving_along(place, offset).wait_recv()
            across(place, offset).start()

    def finish(place):
        for offset in range(planes):
            arriving_across(place, offset).wait_recv()

    def over(row):
        return remote(acts.at[row, :, core], d_send.at[row], d_recv.at[row], other_core)

    def arriving_over(row):
        return remote(acts.at[row, :, 1 - core], d_send.at[row], d_recv.at[row], other_core)

    def load_act(row):
        return pltpu.make_async_copy(
            act.at[core, :, pl.ds(row * BLK, BLK)], acts.at[row, me, core], load_sem.at[row]
        )

    def load_grad(col):
        return pltpu.make_async_copy(
            grad.at[:, pl.ds(col * BLK, BLK)], grads.at[col, me], load_sem.at[row_blocks + col]
        )

    load_act(0).start()
    load_grad(0).start()
    for row in range(1, row_blocks):
        load_act(row).start()
    for col in range(1, col_blocks):
        load_grad(col).start()
    pl.semaphore_wait(barrier, planes + 1)
    load_act(0).wait()
    send_along(act_place(0))
    send_across(act_place(0))
    load_grad(0).wait()
    send_along(grad_place(0))
    send_across(grad_place(0))
    for row in range(1, row_blocks):
        load_act(row).wait()
    for col in range(1, col_blocks):
        load_grad(col).wait()
    pass_on(act_place(0))
    pass_on(grad_place(0))
    for row in range(1, row_blocks):
        send_along(act_place(row))
        send_across(act_place(row))
    send_along(grad_place(1))
    finish(act_place(0))
    over(0).start()
    finish(grad_place(0))
    arriving_over(0).wait_recv()
    total[...] = jnp.zeros_like(total)

    def write_roots(at):
        return pltpu.make_async_copy(root, all_roots.at[at], root_sem)

    def write_update(block_id):
        return pltpu.make_async_copy(update, assembled.at[block_id], update_sem)

    def keep_act(row):
        return pltpu.make_async_copy(acts.at[row], kept_acts.at[row], kept_sem.at[row])

    def keep_grad(index):
        return pltpu.make_async_copy(
            grads.at[trades[index][0]], kept_grads.at[index], kept_sem.at[row_blocks + index]
        )

    def traded(index, theirs):
        col, kind = trades[index]
        row = trader_row(kind, me)
        row = 1 - row if theirs else row
        at = row * col_blocks + col
        return at, remote(
            assembled.at[at], trade_send.at[index], trade_recv.at[index], beside if kind == "y" else facing
        )

    rows, cols, swaps, begins, sent = [], [], [], [], {}
    for col in range(col_blocks):
        kinds = [kind for at, kind in trades if at == col]
        begins.append(len(rows))
        if kinds:
            sent[len(sent)] = len(rows)
            rows.append(trader_row(kinds[0], me))
            swaps.append(swap_of(table, (col, kinds[0]), me, col_blocks, per_owner))
            cols.append(col)
        else:
            rows += list(range(row_blocks))
            swaps += [0] * row_blocks
            cols += [col] * row_blocks
    steps = len(rows)

    @pl.loop(0, steps)
    def _(step):
        if trades:
            held_row, col, swap = pick(step, rows), pick(step, cols), pick(step, swaps)
            row = held_row + swap - 2 * held_row * swap
            first = functools.reduce(jnp.logical_or, [step == at for at in begins[1:]])
        else:
            row, col = lax.rem(step, row_blocks), step // row_blocks
            held_row, first = row, jnp.logical_and(row == 0, step > 0)
        at = held_row * col_blocks + col
        slot = table[0, row * col_blocks + col]

        @pl.when(first)
        def _():
            finish(grad_place(col))

        for other in range(1, row_blocks):
            @pl.when(step == other)
            def _():
                arriving_over(other).wait_recv()

        @pl.when(step > 0)
        def _():
            write_roots(0).wait()

        def between(side):
            @pl.when(jnp.logical_and(side == 1, step == 0))
            def _():
                for other in range(1, row_blocks):
                    pass_on(act_place(other))
                send_across(grad_place(1))
                if col_blocks > 2:
                    send_along(grad_place(2))

            @pl.when(jnp.logical_and(side == 0, step == 1))
            def _():
                pass_on(grad_place(1))
                if col_blocks > 2:
                    send_across(grad_place(2))

            ahead = jnp.logical_and(side == 1, step > 0)

            @pl.when(jnp.logical_and(ahead, step + 1 < col_blocks))
            def _():
                pass_on(grad_place(step + 1))

            @pl.when(jnp.logical_and(ahead, step + 2 < col_blocks))
            def _():
                send_across(grad_place(step + 2))
                send_along(grad_place(step + 2))

            if trades:
                @pl.when(jnp.logical_and(ahead, step == col_blocks - 2))
                def _():
                    traded(0, False)[1].start()

        def form():
            if not trades:
                form_gradient(gradient, acts[row], grads[col])
                return
            trading = functools.reduce(jnp.logical_or, [step == at for at in sent.values()])

            @pl.when(trading)
            def _():
                form_gradient(gradient, acts[row], grads[col])

            @pl.when(jnp.logical_not(trading))
            def _():
                form_gradient(gradient, acts[held_row], grads[col])

        precondition_block(
            form, exponents[0, slot], damping_of(picks[0, slot]),
            gradient, current, factor, second, square, root, between,
        )

        @pl.when(step == 0)
        def _():
            for other in range(1, row_blocks):
                finish(act_place(other))
                over(other).start()

        write_roots(at).start()
        second[...] = dot(root[0], gradient[...]).astype(jnp.bfloat16)
        rounded = dot(second[...], root[1]).astype(jnp.bfloat16)
        total[...] += fold(rounded.astype(jnp.float32))
        if resident:
            assembled[at] = rounded
        else:
            @pl.when(step > 0)
            def _():
                write_update(0).wait()

            update[...] = rounded
            write_update(at).start()
        for index in range(len(trades)):
            @pl.when(step == sent[index])
            def _():
                if index:
                    traded(index, False)[1].start()
                keep_grad(index).start()
                if index < row_blocks:
                    keep_act(index).start()

    for index in range(len(trades)):
        at, copy = traded(index, True)
        copy.wait_recv()
        total[...] += fold(assembled[at].astype(jnp.float32))
    lanes = total[:, :128]
    for start in range(128, BLK, 128):
        lanes = lanes + total[:, start : start + 128]
    own_sum[...] = lanes
    exchange = pltpu.make_async_remote_copy(
        src_ref=own_sum, dst_ref=other_sum, send_sem=s_send, recv_sem=s_recv,
        device_id=other_core, device_id_type=MESH,
    )
    exchange.start()
    write_roots(0).wait()
    if not resident:
        write_update(0).wait()
    for index in range(len(trades)):
        traded(index, False)[1].wait_send()
        keep_grad(index).wait()
        if index < row_blocks:
            keep_act(index).wait()
    for place in [act_place(row) for row in range(row_blocks)] + [grad_place(col) for col in range(col_blocks)]:
        for offset in range(1, planes):
            along(place, offset).wait_send()
        for offset in range(planes):
            across(place, offset).wait_send()
    for row in range(row_blocks):
        over(row).wait_send()
    exchange.wait()
    sums[...] = own_sum[...] + other_sum[...]


def gathered_updates(act, grad, table, exponents, picks, plan, halves):
    owners, row_blocks, col_blocks, per_owner, resident, trades = plan
    tokens, width = act.shape
    blocks, units = row_blocks * col_blocks, row_blocks + col_blocks
    planes = owners // 2
    one = pltpu.VMEM((BLK, BLK), jnp.bfloat16)
    two = pltpu.VMEM((2, BLK, BLK), jnp.bfloat16)
    small = pltpu.VMEM((8, 128), jnp.float32)
    dma = pltpu.SemaphoreType.DMA
    hbm = pl.BlockSpec(memory_space=pl.ANY)
    smem = pl.BlockSpec(memory_space=pltpu.SMEM)
    vmem = pl.BlockSpec(memory_space=pltpu.VMEM)
    acts_shape = (row_blocks, owners, halves, tokens // halves, BLK)
    grads_shape = (col_blocks, owners, tokens, BLK)
    shapes = [
        (pltpu.VMEM if resident else pltpu.HBM)((blocks, BLK, BLK), jnp.bfloat16),
        pltpu.HBM((blocks, 2, BLK, BLK), jnp.bfloat16),
        jax.ShapeDtypeStruct((8, 128), jnp.float32),
    ]
    specs = [vmem if resident else hbm, hbm, vmem]
    if trades:
        shapes += [
            pltpu.HBM(acts_shape, jnp.bfloat16),
            pltpu.HBM((len(trades),) + grads_shape[1:], jnp.bfloat16),
        ]
        specs += [hbm, hbm]
    scratch = [
        pltpu.VMEM(acts_shape, jnp.bfloat16), pltpu.VMEM(grads_shape, jnp.bfloat16),
        one, one, one, one, two, two, pltpu.VMEM((8, BLK), jnp.float32), small, small,
    ]
    sems = [
        dma((units,)), dma((units, planes)), dma((units, planes)),
        dma((units, planes)), dma((units, planes)), dma((row_blocks,)), dma((row_blocks,)),
        dma, dma, dma,
    ]
    if not resident:
        scratch, sems = scratch + [one], sems + [dma]
    if trades:
        sems += [dma((row_blocks + len(trades),)), dma((len(trades),)), dma((len(trades),))]
    return pl.pallas_call(
        functools.partial(gather_kernel, plan),
        out_shape=tuple(shapes),
        in_specs=[hbm, hbm, smem, smem, smem],
        out_specs=tuple(specs),
        scratch_shapes=scratch + sems,
        compiler_params=pltpu.CompilerParams(
            collective_id=0, has_side_effects=True,
            vmem_limit_bytes=RESIDENT_LIMIT if resident else VMEM_BYTES,
        ),
        cost_estimate=pl.CostEstimate(
            flops=blocks * 26 * BLK**3, bytes_accessed=blocks * 6 * BLK**2, transcendentals=0
        ),
        name="gathered_updates",
    )(act.reshape(halves, tokens // halves, width), grad, table, exponents, picks)


def empty_root(quartic, damping):
    def narrow(value):
        return value.astype(jnp.bfloat16).astype(jnp.float32)

    ones = jnp.ones((8, 128), jnp.float32)
    order = jnp.where(quartic == 1, 4.0, 2.0)
    inverse_order = jnp.where(quartic == 1, 0.25, 0.5)
    start = ones * (damping * (BLK / (2.0 * (BLK * damping))))
    factor = narrow((order + 1.0 - start) * inverse_order)
    square = narrow(factor * factor)
    raised = jnp.where(quartic == 1, narrow(square * square), square)
    second = narrow((order + 1.0 - raised * narrow(start)) * inverse_order)
    return (factor * second)[:1, :1]


def finish_kernel(plan, count, *refs):
    owners, row_blocks, col_blocks, per_owner, resident, trades = plan
    ints, table, exponents, picks, sums, unscaled, all_roots = refs[:7]
    refs = refs[7:]
    if trades:
        kept_acts, kept_grads = refs[:2]
        refs = refs[2:]
    out, roots_out, stage, roots, progress, stage_sem, root_load, root_store = refs[:8]
    if not resident:
        piece, piece_sem = refs[8:]
    if trades:
        act, grad, gradient, current, factor, second, square, kept_sem = refs[8:]
    blocks = row_blocks * col_blocks
    depth, rows = stage.shape[0], stage.shape[1]
    parts = BLK // rows
    me = ints[per_owner]
    rescale = lax.rsqrt(jnp.full((8, 128), jnp.sum(sums[...]) / count + 1.0, jnp.float32))[:1, :1]

    def block_of(which):
        return jnp.maximum(ints[which] - 1, 0)

    def held_at(block_id):
        row, col = block_id // col_blocks, lax.rem(block_id, col_blocks)
        swap, absent = jnp.int32(0), jnp.bool_(False)
        for trade in trades:
            here = col == trade[0]
            swap = jnp.where(here, swap_of(table, trade, me, col_blocks, per_owner), swap)
        row = row + swap - 2 * row * swap
        for at, kind in trades:
            absent = jnp.logical_or(absent, jnp.logical_and(col == at, row != trader_row(kind, me)))
        return row * col_blocks + col, absent

    def missing(which):
        return jnp.logical_and(ints[which] > 0, held_at(block_of(which))[1])

    def ready(which):
        return jnp.logical_and(ints[which] > 0, jnp.logical_not(missing(which)))

    def load_roots(which):
        return pltpu.make_async_copy(all_roots.at[held_at(block_of(which))[0]], roots.at[which], root_load.at[which])

    def store_roots(which):
        return pltpu.make_async_copy(roots.at[which], roots_out.at[which], root_store.at[which])

    def store_piece(index, slot):
        block_id = held_at(index // parts)[0]
        at_row = (block_id // col_blocks) * BLK + lax.rem(index, parts) * rows
        at_col = lax.rem(block_id, col_blocks) * BLK
        to = out.at[pl.ds(pl.multiple_of(at_row, rows), rows), pl.ds(pl.multiple_of(at_col, BLK), BLK)]
        return pltpu.make_async_copy(stage.at[slot], to, stage_sem.at[slot])

    for which in range(per_owner):
        @pl.when(ready(which))
        def _():
            load_roots(which).start()

    def scale_pieces(first, stop):
        @pl.loop(first, stop)
        def _(index):
            slot = lax.rem(index, depth)

            @pl.when(index >= depth)
            def _():
                store_piece(index, slot).wait()

            at = pl.ds(pl.multiple_of(lax.rem(index, parts) * rows, rows), rows)
            if resident:
                values = unscaled[index // parts, at]
            else:
                load = pltpu.make_async_copy(unscaled.at[index // parts, at], piece, piece_sem)
                load.start()
                load.wait()
                values = piece[...]
            stage[slot] = (values.astype(jnp.float32) * rescale).astype(jnp.bfloat16)
            store_piece(index, slot).start()

    pieces = blocks * parts
    progress[0] = 0

    def scale_some(share):
        first = progress[0]
        stop = jnp.minimum(first + share, pieces)
        scale_pieces(first, stop)
        progress[0] = stop

    scale_some(depth)
    for which in range(per_owner):
        @pl.when(ready(which))
        def _():
            load_roots(which).wait()
            store_roots(which).start()

        @pl.when(ints[which] == 0)
        def _():
            slot = me * per_owner + which
            value = empty_root(exponents[slot], damping_of(picks[slot]))
            for start in range(0, BLK, PANEL):
                row = lax.broadcasted_iota(jnp.int32, (PANEL, BLK), 0) + start
                diagonal = row == lax.broadcasted_iota(jnp.int32, (PANEL, BLK), 1)
                for side in range(2):
                    roots[which, side, start : start + PANEL, :] = jnp.where(
                        diagonal, value, 0.0
                    ).astype(jnp.bfloat16)
            store_roots(which).start()

    if trades:
        @pl.loop(0, per_owner)
        def _(which):
            @pl.when(missing(which))
            def _():
                block_id = block_of(which)
                col, at = lax.rem(block_id, col_blocks), jnp.int32(0)
                for index, trade in enumerate(trades):
                    at = jnp.where(col == trade[0], index, at)
                loads = [
                    pltpu.make_async_copy(kept_acts.at[block_id // col_blocks], act, kept_sem.at[0]),
                    pltpu.make_async_copy(kept_grads.at[at], grad, kept_sem.at[1]),
                ]
                for load in loads:
                    load.start()
                for load in loads:
                    load.wait()
                slot = me * per_owner + which
                precondition_block(
                    lambda: form_gradient(gradient, act[...], grad[...]), exponents[slot], damping_of(picks[slot]),
                    gradient, current, factor, second, square, roots.at[which],
                    lambda side: scale_some((pieces - depth + 1) // 2),
                )
                store_roots(which).start()

    scale_some(pieces)
    for slot in range(depth):
        store_piece(slot, slot).wait()
    for which in range(per_owner):
        store_roots(which).wait()


def finish(ints, table, exponents, picks, gathered, plan, count):
    owners, row_blocks, col_blocks, per_owner, resident, trades = plan
    unscaled, all_roots, sums = gathered[:3]
    if resident:
        unscaled = pltpu.with_memory_space_constraint(unscaled, pltpu.VMEM)
    one = pltpu.VMEM((BLK, BLK), jnp.bfloat16)
    two = pltpu.VMEM((2, BLK, BLK), jnp.bfloat16)
    dma = pltpu.SemaphoreType.DMA
    hbm = pl.BlockSpec(memory_space=pl.ANY)
    smem = pl.BlockSpec(memory_space=pltpu.SMEM)
    vmem = pl.BlockSpec(memory_space=pltpu.VMEM)
    depth, rows = 12, 256
    scratch = [
        pltpu.VMEM((depth, rows, BLK), jnp.bfloat16),
        pltpu.VMEM((per_owner, 2, BLK, BLK), jnp.bfloat16),
        pltpu.SMEM((1,), jnp.int32), dma((depth,)), dma((per_owner,)), dma((per_owner,)),
    ]
    if not resident:
        scratch += [pltpu.VMEM((rows, BLK), jnp.bfloat16), dma]
    if trades:
        kept_acts, kept_grads = gathered[3:]
        scratch += [
            pltpu.VMEM(kept_acts.shape[1:], jnp.bfloat16), pltpu.VMEM(kept_grads.shape[1:], jnp.bfloat16),
            one, one, one, one, two, dma((2,)),
        ]
    return pl.pallas_call(
        functools.partial(finish_kernel, plan, count),
        out_shape=(
            jax.ShapeDtypeStruct((row_blocks * BLK, col_blocks * BLK), jnp.bfloat16),
            jax.ShapeDtypeStruct((per_owner, 2, BLK, BLK), jnp.bfloat16),
        ),
        in_specs=[smem, smem, smem, smem, vmem, vmem if resident else hbm, hbm] + [hbm] * (len(gathered) - 3),
        out_specs=(hbm, hbm),
        scratch_shapes=scratch,
        compiler_params=pltpu.CompilerParams(vmem_limit_bytes=RESIDENT_LIMIT),
        cost_estimate=pl.CostEstimate(
            flops=10**9, bytes_accessed=4 * row_blocks * col_blocks * BLK**2, transcendentals=0
        ),
        name="scaled_update",
    )(ints, table, exponents, picks, sums, unscaled, all_roots, *gathered[3:])


def on_device(activations, out_grads, slot_table, exponent_index, damping_index):
    half_width = out_grads.shape[1]
    half_blocks = (activations.shape[1] // BLK) * (half_width // BLK)
    owners = lax.axis_size("dp")
    halves = lax.axis_size("mp")
    per_owner = slot_table.shape[1] // owners
    me = lax.axis_index("dp")

    places = jnp.arange(per_owner + 1, dtype=jnp.int32)
    matches = slot_table[0, :half_blocks][None, :] == (me * per_owner + places)[:, None]
    held = jnp.sum(jnp.where(matches, jnp.arange(1, half_blocks + 1, dtype=jnp.int32)[None, :], 0), axis=1)
    ints = jnp.where(places == per_owner, me, held).astype(jnp.int32)

    row_blocks, col_blocks = activations.shape[1] // BLK, half_width // BLK
    tokens = activations.shape[0] * owners
    inputs = 2 * tokens * (activations.shape[1] + half_width)
    resident = inputs + 2 * (half_blocks + 10) * BLK * BLK <= RESIDENT_BYTES
    trades = ()
    if resident and row_blocks == 2 and col_blocks > 4 and owners % 4 == 0:
        trades = ((1, "z"), (2, "y"), (3, "z"))
    plan = (owners, row_blocks, col_blocks, per_owner, resident, trades)
    gathered = gathered_updates(
        activations, out_grads, slot_table, exponent_index, damping_index, plan, halves
    )
    count = float(activations.shape[1] * half_width * halves)
    update, roots = finish(ints, slot_table, exponent_index[0], damping_index[0], gathered, plan, count)
    return (update, roots[None])


def solution(mesh):
    placed = (
        P(("member", "dp"), None),
        P(("member", "dp"), "mp"),
        P(("member", "mp"), None),
        P(("member", "mp"), None),
        P(("member", "mp"), None),
    )
    return jax.shard_map(
        on_device,
        mesh=mesh,
        in_specs=placed,
        out_specs=(P("member", "mp"), P(("member", "mp"), "dp", None, None, None)),
        check_vma=False,
    )
```
